1024 devices in a mesh: gx: 16 (over x, core), gy: 8 (over z), gz: 8 (over y).
Axes of the slice: x: 8, y: 8, z: 8, core: 2. Of those that a mesh axis runs over, the one named last changes fastest.
Arguments:
- field: float32 [256, 128, 1024], P('gx', 'gz', 'gy'), may hold values from -6 to 6
Outputs:
- coefficients: float32 [256, 128, 1024], P('gx', 'gz', 'gy')
The draws below stay inside these ranges and needn't reach their ends.
All inputs are finite; a program needn't handle non-finite values.
Results may differ from the reference program's by a relative error of at most 0.00002.
Values sent between devices are 32-bit elements; how exact they have to be, the bound alone decides.
No kernel may reach another device: no remote copies, remote signals or barrier semaphores. Data moves between devices by JAX's collectives and lax.ppermute only.
A program may use at most 32 MiB of HBM per device.

```python
import jax
import jax.numpy as jnp
from jax import lax

NX = 256
NY = 1024
NZ = 128


def levels(rng, shape, cuts, low, high):
    loudness = 1.0
    for position, blocks in cuts:
        steps = jax.random.uniform(jax.random.fold_in(jax.random.fold_in(rng, 6), position), (blocks,), jnp.float32, low / len(cuts), high / len(cuts))
        loudness = loudness * jnp.repeat(jnp.exp(steps), shape[position] // blocks).reshape((-1,) + (1,) * (len(shape) - 1 - position))
    return loudness


def noise(stream_key, dims, deviation, limit, pieces=(), held_as=jnp.bfloat16):
    loudness = levels(stream_key, dims, pieces, -0.22, 0.18) if pieces else 1.0
    values = jax.random.normal(stream_key, dims, jnp.float32) * deviation * loudness
    return jnp.minimum(jnp.maximum(values, -limit), limit).astype(held_as)


def setup_inputs(seed: int = 0) -> dict:
    key_list = jax.random.split(jax.random.key(seed), 2)
    return {
        "field": noise(key_list[0], (NX, NZ, NY), 1.0, 6.0, ((0, 16), (1, 8), (2, 8)), jnp.float32),
    }


ALPHA = -1.586134342
BETA = -0.05298011854
GAMMA = 0.8829110762
DELTA = 0.4435068522
ZETA = 1.149604398


def piece(array, start, stop, dim):
    return lax.slice_in_dim(array, start, stop, axis=dim)


def lift_padded(padded, dim):
    total = padded.shape[dim]
    half = total // 2
    shape = padded.shape[:dim] + (half, 2) + padded.shape[dim + 1:]
    pairs = padded.reshape(shape)
    even = lax.index_in_dim(pairs, 0, dim + 1, keepdims=False)
    odd = lax.index_in_dim(pairs, 1, dim + 1, keepdims=False)
    odd_one = piece(odd, 0, half - 1, dim) + ALPHA * (piece(even, 0, half - 1, dim) + piece(even, 1, half, dim))
    even_two = piece(even, 1, half - 1, dim) + BETA * (piece(odd_one, 0, half - 2, dim) + piece(odd_one, 1, half - 1, dim))
    odd_three = piece(odd_one, 1, half - 2, dim) + GAMMA * (piece(even_two, 0, half - 3, dim) + piece(even_two, 1, half - 2, dim))
    even_four = piece(even_two, 1, half - 3, dim) + DELTA * (piece(odd_three, 0, half - 4, dim) + piece(odd_three, 1, half - 3, dim))
    lowpass = even_four * ZETA
    highpass = piece(odd_three, 1, half - 3, dim) / ZETA
    joined = jnp.stack([lowpass, highpass], axis=dim + 1)
    out_shape = padded.shape[:dim] + (total - 8,) + padded.shape[dim + 1:]
    return joined.reshape(out_shape)


def lift_axis(array, dim):
    widths = [(0, 0)] * array.ndim
    widths[dim] = (4, 4)
    return lift_padded(jnp.pad(array, widths, mode="reflect"), dim)


def lift_three(array):
    for dim in range(3):
        array = lift_axis(array, dim)
    return array


def reference(field):
    level_one = lift_three(field)
    coarse = level_one[::2, ::2, ::2]
    level_two = lift_three(coarse)
    return level_one.at[::2, ::2, ::2].set(level_two)
```

```python
import jax
import jax.numpy as jnp
import numpy as np
from jax import lax
from jax.experimental import pallas as pl
from jax.experimental.pallas import tpu as pltpu
from jax.sharding import PartitionSpec as P

ALPHA = -1.586134342
BETA = -0.05298011854
GAMMA = 0.8829110762
DELTA = 0.4435068522
ZETA = 1.149604398

BLOCK = 16
LANES = 128
EDGE = 16


def lift_rows(rows, first, last):
    state = dict(rows)
    lo = first + (first & 1)
    hi = last - (last & 1)
    reach = 1
    for parity, weight in ((1, ALPHA), (0, BETA), (1, GAMMA), (0, DELTA)):
        for i in range(lo + reach, hi - reach + 1):
            if (i & 1) == parity:
                state[i] = state[i] + weight * (state[i - 1] + state[i + 1])
        reach += 1
    return state, lo + 4, hi - 4


def both_levels(rows, low, high, is_last):
    state, start, stop = lift_rows(rows, -low, BLOCK - 1 + high)
    coarse = {i // 2: state[i] * ZETA for i in range(start, stop + 1) if not i & 1}
    return coarse, second_level(coarse, is_last)


def second_level(coarse, is_last):
    half = BLOCK // 2
    coarse = dict(coarse)
    for j in range(3):
        coarse[half + j] = jnp.where(is_last, coarse[half - 2 - j], coarse[half + j])
    state, _, _ = lift_rows(coarse, -4, half + 2)
    return finish(state, half)


def finish(state, count):
    return [state[i] * (1.0 / ZETA) if i & 1 else state[i] * ZETA for i in range(count)]


def lift_matrix(padded):
    even, odd = padded[0::2], padded[1::2]
    odd = odd[:-1] + ALPHA * (even[:-1] + even[1:])
    even = even[1:-1] + BETA * (odd[:-1] + odd[1:])
    odd = odd[1:-1] + GAMMA * (even[:-1] + even[1:])
    even = even[1:-1] + DELTA * (odd[:-1] + odd[1:])
    out = np.zeros((2 * len(even), padded.shape[1]))
    out[0::2] = even * ZETA
    out[1::2] = odd[1:] / ZETA
    return out


def y_matrices():
    n, wide = LANES, 24
    size = n + 2 * wide
    eye = np.eye(size)
    own = eye[wide : wide + n]

    def levels(ext, last):
        one = lift_matrix(ext)
        low = one[0::2]
        if last:
            half = n // 2
            low = low.copy()
            for j in range(8):
                low[10 + half + j] = low[10 + half - 2 - j]
        two = lift_matrix(low[: len(low) - len(low) % 2])
        fine = np.zeros((n, size))
        fine[0::2] = two[6 : 6 + n // 2]
        return one[20 : 20 + n], fine

    inner = levels(eye, False)
    left = eye.copy()
    left[:wide] = own[1 : wide + 1][::-1]
    first = levels(left, False)
    right = eye.copy()
    right[wide + n :] = own[n - 1 - wide : n - 1][::-1]
    final = levels(right, True)
    mains, edges = [], []
    for a, b, c in zip(inner, first, final):
        a, b, c = a.T, b.T, c.T
        mid = a[wide : wide + n]
        edges.append(
            np.stack(
                [
                    a[wide - EDGE : wide],
                    (b - a)[wide : wide + EDGE],
                    a[wide + n : wide + n + EDGE],
                    (c - a)[wide + n - EDGE : wide + n],
                ]
            )
        )
        mains.append(mid)
    return np.stack(mains).astype(np.float32), np.stack(edges).astype(np.float32)


MAINS, EDGES = y_matrices()


def x_kernel(field, low, high, one, two, up, down):
    where = lax.axis_index("gx")
    is_first, is_last = where == 0, where == lax.axis_size("gx") - 1
    rows = {i: field[i] for i in range(BLOCK)}
    own = dict(rows)
    for k in range(1, 13):
        rows[-k] = jnp.where(is_first, own[k], low[12 - k])
    for k in range(1, 10):
        rows[BLOCK - 1 + k] = jnp.where(is_last, own[BLOCK - 1 - k], high[k - 1])
    state, _, _ = lift_rows(rows, -12, BLOCK + 8)
    coarse = {i // 2: state[i] * ZETA for i in range(-8, BLOCK + 5, 2)}
    for i, row in enumerate(finish(state, BLOCK)):
        one[i * BLOCK : (i + 1) * BLOCK, :] = row
    for i, row in enumerate(second_level(coarse, is_last)):
        two[i * BLOCK : (i + 1) * BLOCK, :] = row
    half = BLOCK // 2
    for j in range(4):
        up[j * BLOCK : (j + 1) * BLOCK, :] = one[pl.ds(BLOCK - 4 + j, BLOCK, stride=BLOCK), :]
    for j in range(12):
        up[4 * BLOCK + j * half : 4 * BLOCK + (j + 1) * half, :] = two[pl.ds(BLOCK - 12 + j, half, stride=BLOCK), :]
    for j in range(3):
        down[j * BLOCK : (j + 1) * BLOCK, :] = one[pl.ds(j, BLOCK, stride=BLOCK), :]
    for j in range(9):
        down[3 * BLOCK + j * half : 3 * BLOCK + (j + 1) * half, :] = two[pl.ds(j, half, stride=BLOCK), :]


def z_kernel(one, two, low, high, both, up, down):
    where = lax.axis_index("gz")
    is_first, is_last = where == 0, where == lax.axis_size("gz") - 1
    half = BLOCK // 2
    rows = {i: one[pl.ds(i, BLOCK, stride=BLOCK), :] for i in range(BLOCK)}
    own = dict(rows)
    for k in range(1, 5):
        rows[-k] = jnp.where(is_first, own[k], low[(4 - k) * BLOCK : (5 - k) * BLOCK, :])
    for k in range(1, 4):
        rows[BLOCK - 1 + k] = jnp.where(is_last, own[BLOCK - 1 - k], high[(k - 1) * BLOCK : k * BLOCK, :])
    state, _, _ = lift_rows(rows, -4, BLOCK + 2)
    parts = finish(state, BLOCK)
    rows = {i: two[pl.ds(i, half, stride=BLOCK), :] for i in range(BLOCK)}
    own = dict(rows)
    for k in range(1, 13):
        at = 4 * BLOCK + (12 - k) * half
        rows[-k] = jnp.where(is_first, own[k], low[at : at + half, :])
    for k in range(1, 10):
        at = 3 * BLOCK + (k - 1) * half
        rows[BLOCK - 1 + k] = jnp.where(is_last, own[BLOCK - 1 - k], high[at : at + half, :])
    state, _, _ = lift_rows(rows, -12, BLOCK + 8)
    coarse = {i // 2: state[i] * ZETA for i in range(-8, BLOCK + 5, 2)}
    parts += second_level(coarse, is_last)
    parts.append(jnp.zeros((64, LANES), jnp.float32))
    whole = jnp.concatenate(parts, axis=0)
    both[...] = whole
    turned = whole.T
    up[...] = turned[LANES - EDGE :, :]
    down[...] = turned[:EDGE, :]


def y_kernel(both, low, high, up, down, mains, edges, out):
    where = lax.axis_index("gy")
    is_first, is_last = where == 0, where == lax.axis_size("gy") - 1
    cells, half = BLOCK * BLOCK, BLOCK // 2
    ends = jnp.concatenate(
        [jnp.where(is_first, down[...], low[...]), jnp.where(is_last, up[...], high[...])], axis=0
    ).T

    def pass_y(k, start, stop):
        weights = jnp.concatenate(
            [jnp.where(is_first, edges[k, 1], edges[k, 0]), jnp.where(is_last, edges[k, 3], edges[k, 2])], axis=0
        )
        return jnp.dot(
            both[start:stop, :], mains[k], precision=lax.Precision.HIGHEST, preferred_element_type=jnp.float32
        ) + jnp.dot(
            ends[start:stop, :], weights, precision=lax.Precision.HIGHEST, preferred_element_type=jnp.float32
        )

    one = pass_y(0, 0, cells)
    two = pass_y(1, cells, cells + half * half)
    even = (lax.broadcasted_iota(jnp.int32, (half, LANES), 1) & 1) == 0
    for z in range(BLOCK):
        out[pl.ds(z, BLOCK, stride=BLOCK), :] = one[z * BLOCK : (z + 1) * BLOCK, :]
    for z in range(half):
        at = pl.ds(2 * z, half, stride=2 * BLOCK)
        out[at, :] = jnp.where(even, two[z * half : (z + 1) * half, :], out[at, :])


def call(kernel, shapes, *args):
    return pl.pallas_call(
        kernel,
        out_shape=[jax.ShapeDtypeStruct(s, jnp.float32) for s in shapes],
        name=kernel.__name__,
    )(*args)


def exchange(up, down, axis):
    count = lax.axis_size(axis)
    forward = [(i, i + 1) for i in range(count - 1)]
    backward = [(target, source) for source, target in forward]
    high = lax.ppermute(down, axis, backward)
    low = lax.ppermute(up, axis, forward)
    return low, high


def on_device(field):
    cells, half = BLOCK * BLOCK, BLOCK // 2
    low, high = exchange(field[BLOCK - 12 :], field[:9], "gx")
    one, two, up, down = call(
        x_kernel,
        [(cells, LANES), (half * BLOCK, LANES), (4 * BLOCK + 12 * half, LANES), (3 * BLOCK + 9 * half, LANES)],
        field,
        low,
        high,
    )
    low, high = exchange(up, down, "gz")
    wide = cells + 128
    both, up, down = call(z_kernel, [(wide, LANES), (EDGE, wide), (EDGE, wide)], one, two, low, high)
    low, high = exchange(up, down, "gy")
    (out,) = call(y_kernel, [(cells, LANES)], both, low, high, up, down, jnp.asarray(MAINS), jnp.asarray(EDGES))
    return out.reshape(BLOCK, BLOCK, LANES)


def solution(mesh):
    placed = (P("gx", "gz", "gy"),)
    return jax.shard_map(
        on_device, mesh=mesh, in_specs=placed, out_specs=P("gx", "gz", "gy"), check_vma=False
    )
```

```python
import jax
import jax.numpy as jnp
import numpy as np
from jax import lax
from jax.experimental import pallas as pl
from jax.experimental.pallas import tpu as pltpu
from jax.sharding import PartitionSpec as P

ALPHA = -1.586134342
BETA = -0.05298011854
GAMMA = 0.8829110762
DELTA = 0.4435068522
ZETA = 1.149604398

BLOCK = 16
LANES = 128
EDGE = 16


def lift_rows(rows, first, last):
    state = dict(rows)
    lo = first + (first & 1)
    hi = last - (last & 1)
    reach = 1
    for parity, weight in ((1, ALPHA), (0, BETA), (1, GAMMA), (0, DELTA)):
        for i in range(lo + reach, hi - reach + 1):
            if (i & 1) == parity:
                state[i] = state[i] + weight * (state[i - 1] + state[i + 1])
        reach += 1
    return state, lo + 4, hi - 4


def second_level(coarse, is_last):
    half = BLOCK // 2
    coarse = dict(coarse)
    for j in range(3):
        coarse[half + j] = jnp.where(is_last, coarse[half - 2 - j], coarse[half + j])
    state, _, _ = lift_rows(coarse, -4, half + 2)
    return finish(state, half)


def finish(state, count):
    return [state[i] * (1.0 / ZETA) if i & 1 else state[i] * ZETA for i in range(count)]


def lift_matrix(padded):
    even, odd = padded[0::2], padded[1::2]
    odd = odd[:-1] + ALPHA * (even[:-1] + even[1:])
    even = even[1:-1] + BETA * (odd[:-1] + odd[1:])
    odd = odd[1:-1] + GAMMA * (even[:-1] + even[1:])
    even = even[1:-1] + DELTA * (odd[:-1] + odd[1:])
    out = np.zeros((2 * len(even), padded.shape[1]))
    out[0::2] = even * ZETA
    out[1::2] = odd[1:] / ZETA
    return out


def y_matrices():
    n, wide = LANES, 24
    size = n + 2 * wide
    eye = np.eye(size)
    own = eye[wide : wide + n]

    def levels(ext, last):
        one = lift_matrix(ext)
        low = one[0::2]
        if last:
            half = n // 2
            low = low.copy()
            for j in range(8):
                low[10 + half + j] = low[10 + half - 2 - j]
        two = lift_matrix(low[: len(low) - len(low) % 2])
        fine = np.zeros((n, size))
        fine[0::2] = two[6 : 6 + n // 2]
        return one[20 : 20 + n], fine

    inner = levels(eye, False)
    left = eye.copy()
    left[:wide] = own[1 : wide + 1][::-1]
    first = levels(left, False)
    right = eye.copy()
    right[wide + n :] = own[n - 1 - wide : n - 1][::-1]
    final = levels(right, True)
    mains, edges = [], []
    for a, b, c in zip(inner, first, final):
        a, b, c = a.T, b.T, c.T
        mid = a[wide : wide + n]
        edges.append(
            np.stack(
                [
                    a[wide - EDGE : wide],
                    (b - a)[wide : wide + EDGE],
                    a[wide + n : wide + n + EDGE],
                    (c - a)[wide + n - EDGE : wide + n],
                ]
            )
        )
        mains.append(mid)
    return np.stack(mains).astype(np.float32), np.stack(edges).astype(np.float32)


MAINS, EDGES = y_matrices()


def x_kernel(field, low, high, one, two, up, down):
    where = lax.axis_index("gx")
    is_first, is_last = where == 0, where == lax.axis_size("gx") - 1
    rows = {i: field[i] for i in range(BLOCK)}
    own = dict(rows)
    for k in range(1, 13):
        rows[-k] = jnp.where(is_first, own[k], low[12 - k])
    for k in range(1, 10):
        rows[BLOCK - 1 + k] = jnp.where(is_last, own[BLOCK - 1 - k], high[k - 1])
    state, _, _ = lift_rows(rows, -12, BLOCK + 8)
    coarse = {i // 2: state[i] * ZETA for i in range(-8, BLOCK + 5, 2)}
    for i, row in enumerate(finish(state, BLOCK)):
        one[i * BLOCK : (i + 1) * BLOCK, :] = row
    for i, row in enumerate(second_level(coarse, is_last)):
        two[i * BLOCK : (i + 1) * BLOCK, :] = row
    half = BLOCK // 2
    for j in range(4):
        up[j * BLOCK : (j + 1) * BLOCK, :] = one[pl.ds(BLOCK - 4 + j, BLOCK, stride=BLOCK), :]
    for j in range(12):
        up[4 * BLOCK + j * half : 4 * BLOCK + (j + 1) * half, :] = two[pl.ds(BLOCK - 12 + j, half, stride=BLOCK), :]
    for j in range(3):
        down[j * BLOCK : (j + 1) * BLOCK, :] = one[pl.ds(j, BLOCK, stride=BLOCK), :]
    for j in range(9):
        down[3 * BLOCK + j * half : 3 * BLOCK + (j + 1) * half, :] = two[pl.ds(j, half, stride=BLOCK), :]


def z_kernel(one, two, low, high, both, up, down):
    where = lax.axis_index("gz")
    is_first, is_last = where == 0, where == lax.axis_size("gz") - 1
    half = BLOCK // 2
    rows = {i: one[pl.ds(i, BLOCK, stride=BLOCK), :] for i in range(BLOCK)}
    own = dict(rows)
    for k in range(1, 5):
        rows[-k] = jnp.where(is_first, own[k], low[(4 - k) * BLOCK : (5 - k) * BLOCK, :])
    for k in range(1, 4):
        rows[BLOCK - 1 + k] = jnp.where(is_last, own[BLOCK - 1 - k], high[(k - 1) * BLOCK : k * BLOCK, :])
    state, _, _ = lift_rows(rows, -4, BLOCK + 2)
    parts = finish(state, BLOCK)
    rows = {i: two[pl.ds(i, half, stride=BLOCK), :] for i in range(BLOCK)}
    own = dict(rows)
    for k in range(1, 13):
        at = 4 * BLOCK + (12 - k) * half
        rows[-k] = jnp.where(is_first, own[k], low[at : at + half, :])
    for k in range(1, 10):
        at = 3 * BLOCK + (k - 1) * half
        rows[BLOCK - 1 + k] = jnp.where(is_last, own[BLOCK - 1 - k], high[at : at + half, :])
    state, _, _ = lift_rows(rows, -12, BLOCK + 8)
    coarse = {i // 2: state[i] * ZETA for i in range(-8, BLOCK + 5, 2)}
    parts += second_level(coarse, is_last)
    parts.append(jnp.zeros((64, LANES), jnp.float32))
    whole = jnp.concatenate(parts, axis=0)
    both[...] = whole
    turned = whole.T
    up[...] = turned[LANES - EDGE :, :]
    down[...] = turned[:EDGE, :]


def y_kernel(both, low, high, up, down, mains, edges, out):
    where = lax.axis_index("gy")
    is_first, is_last = where == 0, where == lax.axis_size("gy") - 1
    cells, half = BLOCK * BLOCK, BLOCK // 2
    ends = jnp.concatenate(
        [jnp.where(is_first, down[...], low[...]), jnp.where(is_last, up[...], high[...])], axis=0
    ).T

    def pass_y(k, start, stop):
        weights = jnp.concatenate(
            [jnp.where(is_first, edges[k, 1], edges[k, 0]), jnp.where(is_last, edges[k, 3], edges[k, 2])], axis=0
        )
        return jnp.dot(
            both[start:stop, :], mains[k], precision=lax.Precision.HIGHEST, preferred_element_type=jnp.float32
        ) + jnp.dot(
            ends[start:stop, :], weights, precision=lax.Precision.HIGHEST, preferred_element_type=jnp.float32
        )

    one = pass_y(0, 0, cells)
    two = pass_y(1, cells, cells + half * half)
    even = (lax.broadcasted_iota(jnp.int32, (half, LANES), 1) & 1) == 0
    for z in range(BLOCK):
        out[pl.ds(z, BLOCK, stride=BLOCK), :] = one[z * BLOCK : (z + 1) * BLOCK, :]
    for z in range(half):
        at = pl.ds(2 * z, half, stride=2 * BLOCK)
        out[at, :] = jnp.where(even, two[z * half : (z + 1) * half, :], out[at, :])


def near(shape):
    return pltpu.VMEM(shape, jnp.float32)


def call(kernel, shapes, *args):
    args = [pltpu.with_memory_space_constraint(a, pltpu.VMEM) for a in args]
    return pl.pallas_call(kernel, out_shape=shapes)(*args)


def exchange(up, down, axis):
    count = lax.axis_size(axis)
    forward = [(i, i + 1) for i in range(count - 1)]
    backward = [(target, source) for source, target in forward]
    high = lax.ppermute(down, axis, backward)
    low = lax.ppermute(up, axis, forward)
    return low, high


def on_device(field):
    cells, half = BLOCK * BLOCK, BLOCK // 2
    low, high = exchange(field[BLOCK - 12 :], field[:9], "gx")
    one, two, up, down = call(
        x_kernel,
        [
            near((cells, LANES)),
            near((half * BLOCK, LANES)),
            near((4 * BLOCK + 12 * half, LANES)),
            near((3 * BLOCK + 9 * half, LANES)),
        ],
        field,
        low,
        high,
    )
    low, high = exchange(up, down, "gz")
    wide = cells + 128
    both, up, down = call(z_kernel, [near((wide, LANES)), near((EDGE, wide)), near((EDGE, wide))], one, two, low, high)
    low, high = exchange(up, down, "gy")
    (out,) = call(
        y_kernel,
        [jax.ShapeDtypeStruct((cells, LANES), jnp.float32)],
        both,
        low,
        high,
        up,
        down,
        jnp.asarray(MAINS),
        jnp.asarray(EDGES),
    )
    return out.reshape(BLOCK, BLOCK, LANES)


def solution(mesh):
    placed = (P("gx", "gz", "gy"),)
    return jax.shard_map(
        on_device, mesh=mesh, in_specs=placed, out_specs=P("gx", "gz", "gy"), check_vma=False
    )
```

```python
import jax
import jax.numpy as jnp
import numpy as np
from jax import lax
from jax.experimental import pallas as pl
from jax.experimental.pallas import tpu as pltpu
from jax.sharding import PartitionSpec as P

ALPHA = -1.586134342
BETA = -0.05298011854
GAMMA = 0.8829110762
DELTA = 0.4435068522
ZETA = 1.149604398

BLOCK = 16
LANES = 128
EDGE = 16


STEPS = (ALPHA, BETA, GAMMA, DELTA)


def advance(state, step, index):
    before = max(step - 2, -1) if step > 1 else -1
    side = step - 1
    state[step, index] = state[before, index] + STEPS[step] * (state[side, index - 1] + state[side, index + 1])


def lift(state, spans):
    for step, (first, last) in enumerate(spans):
        for index in range(first, last + 1, 2):
            if (step, index) not in state:
                advance(state, step, index)


UP = ((-1, 15), (-1, 14), (0, 13), (1, 12), (2, 11), (3, 10), (3, 8))
DOWN = ((-1, 0), (0, 1), (1, 2), (2, 3), (3, 4))
MIRROR_LOW = ((-1, 1), (-1, 2), (0, 3), (1, 4), (2, 5), (3, 6), (3, 8))
MIRROR_HIGH = ((-1, 14), (0, 13), (1, 12), (2, 11), (3, 10))
INNER = ((1, 13), (2, 12), (3, 11), (4, 10))
BOTH = ((-1, 15), (-2, 16), (-3, 17), (-4, 18))
ONE = ((-1, 15), (-2, 16), (-1, 15), (0, 14))


def started(rows):
    state = {(-1, i): rows[i] for i in range(BLOCK)}
    lift(state, INNER)
    return state


def joined(state, low, high, is_first, is_last, spans):
    for k, value in enumerate(low):
        step, index = UP[k]
        state[step, index - BLOCK] = jnp.where(is_first, state[MIRROR_LOW[k]], value)
    for k, value in enumerate(high):
        step, index = DOWN[k]
        state[step, index + BLOCK] = jnp.where(is_last, state[MIRROR_HIGH[k]], value)
    lift(state, spans)
    return state


def level_one(state):
    return [state[2, i] * (1.0 / ZETA) if i & 1 else state[3, i] * ZETA for i in range(BLOCK)]


def level_two(state, is_last):
    half = BLOCK // 2
    coarse = {(-1, i): state[3, 2 * i] * ZETA for i in range(-4, half + 3)}
    for j in range(3):
        coarse[-1, half + j] = jnp.where(is_last, coarse[-1, half - 2 - j], coarse[-1, half + j])
    lift(coarse, ((-3, half + 1), (-2, half), (-1, half - 1), (0, half - 2)))
    return [coarse[2, i] * (1.0 / ZETA) if i & 1 else coarse[3, i] * ZETA for i in range(half)]


def lift_matrix(padded):
    even, odd = padded[0::2], padded[1::2]
    odd = odd[:-1] + ALPHA * (even[:-1] + even[1:])
    even = even[1:-1] + BETA * (odd[:-1] + odd[1:])
    odd = odd[1:-1] + GAMMA * (even[:-1] + even[1:])
    even = even[1:-1] + DELTA * (odd[:-1] + odd[1:])
    out = np.zeros((2 * len(even), padded.shape[1]))
    out[0::2] = even * ZETA
    out[1::2] = odd[1:] / ZETA
    return out


def y_matrices():
    n, wide = LANES, 24
    size = n + 2 * wide
    eye = np.eye(size)
    own = eye[wide : wide + n]

    def levels(ext, last):
        one = lift_matrix(ext)
        low = one[0::2]
        if last:
            half = n // 2
            low = low.copy()
            for j in range(8):
                low[10 + half + j] = low[10 + half - 2 - j]
        two = lift_matrix(low[: len(low) - len(low) % 2])
        fine = np.zeros((n, size))
        fine[0::2] = two[6 : 6 + n // 2]
        return one[20 : 20 + n], fine

    inner = levels(eye, False)
    left = eye.copy()
    left[:wide] = own[1 : wide + 1][::-1]
    first = levels(left, False)
    right = eye.copy()
    right[wide + n :] = own[n - 1 - wide : n - 1][::-1]
    final = levels(right, True)
    mains, edges = [], []
    for a, b, c in zip(inner, first, final):
        a, b, c = a.T, b.T, c.T
        mid = a[wide : wide + n]
        edges.append(
            np.stack(
                [
                    a[wide - EDGE : wide],
                    (b - a)[wide : wide + EDGE],
                    a[wide + n : wide + n + EDGE],
                    (c - a)[wide + n - EDGE : wide + n],
                ]
            )
        )
        mains.append(mid)
    return np.stack(mains).astype(np.float32), np.stack(edges).astype(np.float32)


MAINS, EDGES = y_matrices()


def blank_kernel(blank):
    blank[...] = jnp.zeros(blank.shape, jnp.float32)


def x_start_kernel(field, blank, down):
    state = started({i: field[i] for i in range(BLOCK)})
    for k, key in enumerate(DOWN):
        down[k] = state[key]


def x_kernel(field, low, high, one, two, up, down):
    where = lax.axis_index("gx")
    is_first, is_last = where == 0, where == lax.axis_size("gx") - 1
    half = BLOCK // 2
    before = started({i: low[i] for i in range(BLOCK)})
    state = started({i: field[i] for i in range(BLOCK)})
    joined(state, [before[key] for key in UP], [high[k] for k in range(len(DOWN))], is_first, is_last, BOTH)
    for i, row in enumerate(level_one(state)):
        one[i * BLOCK : (i + 1) * BLOCK, :] = row
    for i, row in enumerate(level_two(state, is_last)):
        two[i * BLOCK : (i + 1) * BLOCK, :] = row
    for source, count, ups, downs in ((one, BLOCK, 3, 2), (two, half, 7, 5)):
        state = started({i: source[pl.ds(i, count, stride=BLOCK), :] for i in range(BLOCK)})
        base = 0 if count == BLOCK else 3 * BLOCK
        for k in range(ups):
            up[base + k * count : base + (k + 1) * count, :] = state[UP[k]]
        base = 0 if count == BLOCK else 2 * BLOCK
        for k in range(downs):
            down[base + k * count : base + (k + 1) * count, :] = state[DOWN[k]]


def z_kernel(one, two, low, high, blank, both, up, down):
    where = lax.axis_index("gz")
    is_first, is_last = where == 0, where == lax.axis_size("gz") - 1
    half = BLOCK // 2
    parts = []
    for source, count, ups, downs, spans in ((one, BLOCK, 3, 2, ONE), (two, half, 7, 5, BOTH)):
        state = started({i: source[pl.ds(i, count, stride=BLOCK), :] for i in range(BLOCK)})
        base = 0 if count == BLOCK else 3 * BLOCK
        lows = [low[base + k * count : base + (k + 1) * count, :] for k in range(ups)]
        base = 0 if count == BLOCK else 2 * BLOCK
        highs = [high[base + k * count : base + (k + 1) * count, :] for k in range(downs)]
        joined(state, lows, highs, is_first, is_last, spans)
        parts += level_one(state) if count == BLOCK else level_two(state, is_last)
    parts.append(blank[...])
    whole = jnp.concatenate(parts, axis=0)
    both[...] = whole
    turned = whole.T
    up[...] = turned[LANES - EDGE :, :]
    down[...] = turned[:EDGE, :]


def y_kernel(both, low, high, up, down, mains, edges, out):
    where = lax.axis_index("gy")
    is_first, is_last = where == 0, where == lax.axis_size("gy") - 1
    cells, half = BLOCK * BLOCK, BLOCK // 2
    ends = jnp.concatenate(
        [jnp.where(is_first, down[...], low[...]), jnp.where(is_last, up[...], high[...])], axis=0
    ).T

    def pass_y(k, start, stop):
        weights = jnp.concatenate(
            [jnp.where(is_first, edges[k, 1], edges[k, 0]), jnp.where(is_last, edges[k, 3], edges[k, 2])], axis=0
        )
        return jnp.dot(
            both[start:stop, :], mains[k], precision=lax.Precision.HIGHEST, preferred_element_type=jnp.float32
        ) + jnp.dot(
            ends[start:stop, :], weights, precision=lax.Precision.HIGHEST, preferred_element_type=jnp.float32
        )

    one = pass_y(0, 0, cells)
    two = pass_y(1, cells, cells + half * half)
    even = (lax.broadcasted_iota(jnp.int32, (half, LANES), 1) & 1) == 0
    for z in range(BLOCK):
        out[pl.ds(z, BLOCK, stride=BLOCK), :] = one[z * BLOCK : (z + 1) * BLOCK, :]
    for z in range(half):
        at = pl.ds(2 * z, half, stride=2 * BLOCK)
        out[at, :] = jnp.where(even, two[z * half : (z + 1) * half, :], out[at, :])


def near(shape):
    return pltpu.VMEM(shape, jnp.float32)


def call(kernel, shapes, *args, flops=None):
    args = [pltpu.with_memory_space_constraint(a, pltpu.VMEM) for a in args]
    cost = None if flops is None else pl.CostEstimate(flops=flops, bytes_accessed=4096, transcendentals=0)
    return pl.pallas_call(kernel, out_shape=shapes, cost_estimate=cost)(*args)


def exchange(up, down, axis):
    count = lax.axis_size(axis)
    forward = [(i, i + 1) for i in range(count - 1)]
    backward = [(target, source) for source, target in forward]
    high = lax.ppermute(down, axis, backward)
    low = lax.ppermute(up, axis, forward)
    return low, high


def on_device(field):
    cells, half = BLOCK * BLOCK, BLOCK // 2
    (blank,) = call(blank_kernel, [near((64, LANES))], flops=10**8)
    (down,) = call(x_start_kernel, [near((len(DOWN), BLOCK, LANES))], field, blank)
    low, high = exchange(field, down, "gx")
    one, two, up, down = call(
        x_kernel,
        [
            near((cells, LANES)),
            near((half * BLOCK, LANES)),
            near((3 * BLOCK + 7 * half, LANES)),
            near((2 * BLOCK + 5 * half, LANES)),
        ],
        field,
        low,
        high,
    )
    low, high = exchange(up, down, "gz")
    wide = cells + 128
    both, up, down = call(
        z_kernel, [near((wide, LANES)), near((EDGE, wide)), near((EDGE, wide))], one, two, low, high, blank
    )
    low, high = exchange(up, down, "gy")
    (out,) = call(
        y_kernel,
        [jax.ShapeDtypeStruct((cells, LANES), jnp.float32)],
        both,
        low,
        high,
        up,
        down,
        jnp.asarray(MAINS),
        jnp.asarray(EDGES),
    )
    return out.reshape(BLOCK, BLOCK, LANES)


def solution(mesh):
    placed = (P("gx", "gz", "gy"),)
    return jax.shard_map(
        on_device, mesh=mesh, in_specs=placed, out_specs=P("gx", "gz", "gy"), check_vma=False
    )
```

```python
import jax
import jax.numpy as jnp
import numpy as np
from jax import lax
from jax.experimental import pallas as pl
from jax.experimental.pallas import tpu as pltpu
from jax.sharding import PartitionSpec as P

ALPHA = -1.586134342
BETA = -0.05298011854
GAMMA = 0.8829110762
DELTA = 0.4435068522
ZETA = 1.149604398

BLOCK = 16
LANES = 128
EDGE = 16


STEPS = (ALPHA, BETA, GAMMA, DELTA)


def advance(state, step, index):
    before = max(step - 2, -1) if step > 1 else -1
    side = step - 1
    state[step, index] = state[before, index] + STEPS[step] * (state[side, index - 1] + state[side, index + 1])


def lift(state, spans):
    for step, (first, last) in enumerate(spans):
        for index in range(first, last + 1, 2):
            if (step, index) not in state:
                advance(state, step, index)


UP = ((-1, 15), (-1, 14), (0, 13), (1, 12), (2, 11), (3, 10), (3, 8))
DOWN = ((-1, 0), (0, 1), (1, 2), (2, 3), (3, 4))
MIRROR_LOW = ((-1, 1), (-1, 2), (0, 3), (1, 4), (2, 5), (3, 6), (3, 8))
MIRROR_HIGH = ((-1, 14), (0, 13), (1, 12), (2, 11), (3, 10))
INNER = ((1, 13), (2, 12), (3, 11), (4, 10))
BOTH = ((-1, 15), (-2, 16), (-3, 17), (-4, 18))
ONE = ((-1, 15), (-2, 16), (-1, 15), (0, 14))


def started(rows):
    state = {(-1, i): rows[i] for i in range(BLOCK)}
    lift(state, INNER)
    return state


def joined(state, low, high, is_first, is_last, spans):
    for k, value in enumerate(low):
        step, index = UP[k]
        state[step, index - BLOCK] = jnp.where(is_first, state[MIRROR_LOW[k]], value)
    for k, value in enumerate(high):
        step, index = DOWN[k]
        state[step, index + BLOCK] = jnp.where(is_last, state[MIRROR_HIGH[k]], value)
    lift(state, spans)
    return state


def level_one(state):
    return [state[2, i] * (1.0 / ZETA) if i & 1 else state[3, i] * ZETA for i in range(BLOCK)]


def level_two(state, is_last):
    half = BLOCK // 2
    coarse = {(-1, i): state[3, 2 * i] * ZETA for i in range(-4, half + 3)}
    for j in range(3):
        coarse[-1, half + j] = jnp.where(is_last, coarse[-1, half - 2 - j], coarse[-1, half + j])
    lift(coarse, ((-3, half + 1), (-2, half), (-1, half - 1), (0, half - 2)))
    return [coarse[2, i] * (1.0 / ZETA) if i & 1 else coarse[3, i] * ZETA for i in range(half)]


def lift_matrix(padded):
    even, odd = padded[0::2], padded[1::2]
    odd = odd[:-1] + ALPHA * (even[:-1] + even[1:])
    even = even[1:-1] + BETA * (odd[:-1] + odd[1:])
    odd = odd[1:-1] + GAMMA * (even[:-1] + even[1:])
    even = even[1:-1] + DELTA * (odd[:-1] + odd[1:])
    out = np.zeros((2 * len(even), padded.shape[1]))
    out[0::2] = even * ZETA
    out[1::2] = odd[1:] / ZETA
    return out


def y_matrices():
    n, wide = LANES, 24
    size = n + 2 * wide
    eye = np.eye(size)
    own = eye[wide : wide + n]

    def levels(ext, last):
        one = lift_matrix(ext)
        low = one[0::2]
        if last:
            half = n // 2
            low = low.copy()
            for j in range(8):
                low[10 + half + j] = low[10 + half - 2 - j]
        two = lift_matrix(low[: len(low) - len(low) % 2])
        fine = np.zeros((n, size))
        fine[0::2] = two[6 : 6 + n // 2]
        return one[20 : 20 + n], fine

    inner = levels(eye, False)
    left = eye.copy()
    left[:wide] = own[1 : wide + 1][::-1]
    first = levels(left, False)
    right = eye.copy()
    right[wide + n :] = own[n - 1 - wide : n - 1][::-1]
    final = levels(right, True)
    mains, edges = [], []
    for a, b, c in zip(inner, first, final):
        a, b, c = a.T, b.T, c.T
        mid = a[wide : wide + n]
        edges.append(
            np.stack(
                [
                    a[wide - EDGE : wide],
                    (b - a)[wide : wide + EDGE],
                    a[wide + n : wide + n + EDGE],
                    (c - a)[wide + n - EDGE : wide + n],
                ]
            )
        )
        mains.append(mid)
    return np.stack(mains).astype(np.float32), np.stack(edges).astype(np.float32)


MAINS, EDGES = y_matrices()


def blank_kernel(blank):
    blank[...] = jnp.zeros(blank.shape, jnp.float32)


def x_start_kernel(field, blank, down):
    state = started({i: field[i] for i in range(BLOCK)})
    for k, key in enumerate(DOWN):
        down[k] = state[key]


def x_kernel(field, low, high, one, two, up, down):
    where = lax.axis_index("gx")
    is_first, is_last = where == 0, where == lax.axis_size("gx") - 1
    half = BLOCK // 2
    before = started({i: low[i] for i in range(BLOCK)})
    state = started({i: field[i] for i in range(BLOCK)})
    joined(state, [before[key] for key in UP], [high[k] for k in range(len(DOWN))], is_first, is_last, BOTH)
    for i, row in enumerate(level_one(state)):
        one[i * BLOCK : (i + 1) * BLOCK, :] = row
    for i, row in enumerate(level_two(state, is_last)):
        two[i * BLOCK : (i + 1) * BLOCK, :] = row
    for source, count, ups, downs in ((one, BLOCK, 3, 2), (two, half, 7, 5)):
        state = started({i: source[pl.ds(i, count, stride=BLOCK), :] for i in range(BLOCK)})
        base = 0 if count == BLOCK else 3 * BLOCK
        for k in range(ups):
            up[base + k * count : base + (k + 1) * count, :] = state[UP[k]]
        base = 0 if count == BLOCK else 2 * BLOCK
        for k in range(downs):
            down[base + k * count : base + (k + 1) * count, :] = state[DOWN[k]]


def z_kernel(one, two, low, high, blank, both, up, down):
    where = lax.axis_index("gz")
    is_first, is_last = where == 0, where == lax.axis_size("gz") - 1
    half = BLOCK // 2
    parts = []
    for source, count, ups, downs, spans in ((one, BLOCK, 3, 2, ONE), (two, half, 7, 5, BOTH)):
        state = started({i: source[pl.ds(i, count, stride=BLOCK), :] for i in range(BLOCK)})
        base = 0 if count == BLOCK else 3 * BLOCK
        lows = [low[base + k * count : base + (k + 1) * count, :] for k in range(ups)]
        base = 0 if count == BLOCK else 2 * BLOCK
        highs = [high[base + k * count : base + (k + 1) * count, :] for k in range(downs)]
        joined(state, lows, highs, is_first, is_last, spans)
        parts += level_one(state) if count == BLOCK else level_two(state, is_last)
    parts.append(blank[...])
    whole = jnp.concatenate(parts, axis=0)
    both[...] = whole
    turned = whole.T
    up[...] = turned[LANES - EDGE :, :]
    down[...] = turned[:EDGE, :]


def dot(a, b):
    return jnp.dot(a, b, precision=lax.Precision.HIGHEST, preferred_element_type=jnp.float32)


def y_main_kernel(both, mains, out):
    cells = BLOCK * BLOCK
    out[:cells, :] = dot(both[:cells, :], mains[0])
    out[cells:, :] = dot(both[cells : cells + cells // 4, :], mains[1])


def y_kernel(main, low, high, up, down, edges, out, block, sems):
    where = lax.axis_index("gy")
    is_first, is_last = where == 0, where == lax.axis_size("gy") - 1
    cells, half = BLOCK * BLOCK, BLOCK // 2
    ends = jnp.concatenate(
        [jnp.where(is_first, down[...], low[...]), jnp.where(is_last, up[...], high[...])], axis=0
    ).T
    weights = [
        jnp.concatenate(
            [jnp.where(is_first, edges[k, 1], edges[k, 0]), jnp.where(is_last, edges[k, 3], edges[k, 2])], axis=0
        )
        for k in range(2)
    ]
    even = (lax.broadcasted_iota(jnp.int32, (half, LANES), 1) & 1) == 0
    whole = block.reshape(BLOCK, BLOCK, LANES)
    copies = []
    for part in range(2):
        rows = slice(part * cells // 2, (part + 1) * cells // 2)
        one = main[rows, :] + dot(ends[rows, :], weights[0])
        rows = slice(cells + part * cells // 8, cells + (part + 1) * cells // 8)
        two = main[rows, :] + dot(ends[rows, :], weights[1])
        for z in range(half):
            block[pl.ds(part * half + z, BLOCK, stride=BLOCK), :] = one[z * BLOCK : (z + 1) * BLOCK, :]
        for z in range(half // 2):
            at = pl.ds(part * half + 2 * z, half, stride=2 * BLOCK)
            block[at, :] = jnp.where(even, two[z * half : (z + 1) * half, :], block[at, :])
        span = pl.ds(part * half, half)
        copies.append(pltpu.make_async_copy(whole.at[:, span, :], out.at[:, span, :], sems.at[part]))
        copies[-1].start()
    for copy in copies:
        copy.wait()


def near(shape):
    return pltpu.VMEM(shape, jnp.float32)


def call(kernel, shapes, *args, flops=None):
    args = [pltpu.with_memory_space_constraint(a, pltpu.VMEM) for a in args]
    cost = None if flops is None else pl.CostEstimate(flops=flops, bytes_accessed=4096, transcendentals=0)
    return pl.pallas_call(kernel, out_shape=shapes, cost_estimate=cost)(*args)


def exchange(up, down, axis):
    count = lax.axis_size(axis)
    forward = [(i, i + 1) for i in range(count - 1)]
    backward = [(target, source) for source, target in forward]
    high = lax.ppermute(down, axis, backward)
    low = lax.ppermute(up, axis, forward)
    return low, high


def on_device(field):
    cells, half = BLOCK * BLOCK, BLOCK // 2
    (blank,) = call(blank_kernel, [near((64, LANES))], flops=10**8)
    (down,) = call(x_start_kernel, [near((len(DOWN), BLOCK, LANES))], field, blank)
    low, high = exchange(field, down, "gx")
    one, two, up, down = call(
        x_kernel,
        [
            near((cells, LANES)),
            near((half * BLOCK, LANES)),
            near((3 * BLOCK + 7 * half, LANES)),
            near((2 * BLOCK + 5 * half, LANES)),
        ],
        field,
        low,
        high,
    )
    low, high = exchange(up, down, "gz")
    wide = cells + 128
    both, up, down = call(
        z_kernel, [near((wide, LANES)), near((EDGE, wide)), near((EDGE, wide))], one, two, low, high, blank
    )
    low, high = exchange(up, down, "gy")
    (main,) = call(
        y_main_kernel, [near((cells + cells // 4, LANES))], both, jnp.asarray(MAINS), flops=10**7
    )
    out = pl.pallas_call(
        y_kernel,
        out_shape=jax.ShapeDtypeStruct((BLOCK, BLOCK, LANES), jnp.float32),
        out_specs=pl.BlockSpec(memory_space=pl.ANY),
        scratch_shapes=[pltpu.VMEM((cells, LANES), jnp.float32), pltpu.SemaphoreType.DMA((2,))],
        name="y_kernel",
    )(*(pltpu.with_memory_space_constraint(a, pltpu.VMEM) for a in (main, low, high, up, down, jnp.asarray(EDGES))))
    return out


def solution(mesh):
    placed = (P("gx", "gz", "gy"),)
    return jax.shard_map(
        on_device, mesh=mesh, in_specs=placed, out_specs=P("gx", "gz", "gy"), check_vma=False
    )
```

```python
import itertools

import jax
import jax.numpy as jnp
import numpy as np
from jax import lax
from jax.experimental import pallas as pl
from jax.experimental.pallas import tpu as pltpu
from jax.sharding import PartitionSpec as P

ALPHA = -1.586134342
BETA = -0.05298011854
GAMMA = 0.8829110762
DELTA = 0.4435068522
ZETA = 1.149604398

BLOCK = 16
LANES = 128
EDGE = 16
NEAR = {"gz": (1, 2), "gy": (2, 2)}


STEPS = (ALPHA, BETA, GAMMA, DELTA)


def advance(state, step, index):
    before = max(step - 2, -1) if step > 1 else -1
    side = step - 1
    state[step, index] = state[before, index] + STEPS[step] * (state[side, index - 1] + state[side, index + 1])


def lift(state, spans):
    for step, (first, last) in enumerate(spans):
        for index in range(first, last + 1, 2):
            if (step, index) not in state:
                advance(state, step, index)


UP = ((-1, 15), (-1, 14), (0, 13), (1, 12), (2, 11), (3, 10), (3, 8))
DOWN = ((-1, 0), (0, 1), (1, 2), (2, 3), (3, 4))
MIRROR_LOW = ((-1, 1), (-1, 2), (0, 3), (1, 4), (2, 5), (3, 6), (3, 8))
MIRROR_HIGH = ((-1, 14), (0, 13), (1, 12), (2, 11), (3, 10))
INNER = ((1, 13), (2, 12), (3, 11), (4, 10))
BOTH = ((-1, 15), (-2, 16), (-3, 17), (-4, 18))
ONE = ((-1, 15), (-2, 16), (-1, 15), (0, 14))


def started(rows):
    state = {(-1, i): rows[i] for i in range(BLOCK)}
    lift(state, INNER)
    return state


def joined(state, low, high, is_first, is_last, spans):
    for k, value in enumerate(low):
        step, index = UP[k]
        state[step, index - BLOCK] = jnp.where(is_first, state[MIRROR_LOW[k]], value)
    for k, value in enumerate(high):
        step, index = DOWN[k]
        state[step, index + BLOCK] = jnp.where(is_last, state[MIRROR_HIGH[k]], value)
    lift(state, spans)
    return state


def level_one(state):
    return [state[2, i] * (1.0 / ZETA) if i & 1 else state[3, i] * ZETA for i in range(BLOCK)]


def level_two(state, is_last):
    half = BLOCK // 2
    coarse = {(-1, i): state[3, 2 * i] * ZETA for i in range(-4, half + 3)}
    for j in range(3):
        coarse[-1, half + j] = jnp.where(is_last, coarse[-1, half - 2 - j], coarse[-1, half + j])
    lift(coarse, ((-3, half + 1), (-2, half), (-1, half - 1), (0, half - 2)))
    return [coarse[2, i] * (1.0 / ZETA) if i & 1 else coarse[3, i] * ZETA for i in range(half)]


def lift_matrix(padded):
    even, odd = padded[0::2], padded[1::2]
    odd = odd[:-1] + ALPHA * (even[:-1] + even[1:])
    even = even[1:-1] + BETA * (odd[:-1] + odd[1:])
    odd = odd[1:-1] + GAMMA * (even[:-1] + even[1:])
    even = even[1:-1] + DELTA * (odd[:-1] + odd[1:])
    out = np.zeros((2 * len(even), padded.shape[1]))
    out[0::2] = even * ZETA
    out[1::2] = odd[1:] / ZETA
    return out


def y_matrices():
    n, wide = LANES, 24
    size = n + 2 * wide
    eye = np.eye(size)
    own = eye[wide : wide + n]

    def levels(ext, last):
        one = lift_matrix(ext)
        low = one[0::2]
        if last:
            half = n // 2
            low = low.copy()
            for j in range(8):
                low[10 + half + j] = low[10 + half - 2 - j]
        two = lift_matrix(low[: len(low) - len(low) % 2])
        fine = np.zeros((n, size))
        fine[0::2] = two[6 : 6 + n // 2]
        return one[20 : 20 + n], fine

    inner = levels(eye, False)
    left = eye.copy()
    left[:wide] = own[1 : wide + 1][::-1]
    first = levels(left, False)
    right = eye.copy()
    right[wide + n :] = own[n - 1 - wide : n - 1][::-1]
    final = levels(right, True)
    mains, edges = [], []
    for a, b, c in zip(inner, first, final):
        a, b, c = a.T, b.T, c.T
        mid = a[wide : wide + n]
        edges.append(
            np.stack(
                [
                    a[wide - EDGE : wide],
                    (b - a)[wide : wide + EDGE],
                    a[wide + n : wide + n + EDGE],
                    (c - a)[wide + n - EDGE : wide + n],
                ]
            )
        )
        mains.append(mid)
    return np.stack(mains).astype(np.float32), np.stack(edges).astype(np.float32)


MAINS, EDGES = y_matrices()


def swapped(axis, gx, gy, gz):
    if axis == "gz":
        return (gy < NEAR["gz"][0]) & (gx < NEAR["gz"][1])
    return (gz < NEAR["gy"][0]) & (gx < NEAR["gy"][1])


def here(axis):
    at = {name: lax.axis_index(name) for name in ("gx", "gy", "gz")}
    swap = swapped(axis, **at)
    odd = lax.rem(at[axis], 2) == 1
    return swap & odd, jnp.logical_or(jnp.logical_not(swap), odd)


def blank_kernel(blank):
    blank[...] = jnp.zeros(blank.shape, jnp.float32)


def x_start_kernel(field, blank, down):
    state = started({i: field[i] for i in range(BLOCK)})
    for k, key in enumerate(DOWN):
        down[k] = state[key]


def x_kernel(field, low, high, one, two, send_one, send_two):
    where = lax.axis_index("gx")
    is_first, is_last = where == 0, where == lax.axis_size("gx") - 1
    half = BLOCK // 2
    before = started({i: low[i] for i in range(BLOCK)})
    state = started({i: field[i] for i in range(BLOCK)})
    joined(state, [before[key] for key in UP], [high[k] for k in range(len(DOWN))], is_first, is_last, BOTH)
    for i, row in enumerate(level_one(state)):
        one[i * BLOCK : (i + 1) * BLOCK, :] = row
    for i, row in enumerate(level_two(state, is_last)):
        two[i * BLOCK : (i + 1) * BLOCK, :] = row
    up_first, _ = here("gz")
    for source, count, base, ups, downs in ((one, BLOCK, 0, 3, 2), (two, half, 3 * BLOCK, 7, 5)):
        state = started({i: source[pl.ds(i, count, stride=BLOCK), :] for i in range(BLOCK)})
        for k in range(ups):
            rows = slice(base + k * count, base + (k + 1) * count)
            up, down = state[UP[k]], state[DOWN[min(k, downs - 1)]]
            send_one[rows, :] = jnp.where(up_first, up, down)
            send_two[rows, :] = jnp.where(up_first, down, up)


def z_kernel(one, two, got_one, got_two, blank, both, up, down, send_one, send_two):
    where = lax.axis_index("gz")
    is_first, is_last = where == 0, where == lax.axis_size("gz") - 1
    half = BLOCK // 2
    _, high_first = here("gz")
    parts = []
    for source, count, base, ups, downs, spans in ((one, BLOCK, 0, 3, 2, ONE), (two, half, 3 * BLOCK, 7, 5, BOTH)):
        state = started({i: source[pl.ds(i, count, stride=BLOCK), :] for i in range(BLOCK)})
        rows = [slice(base + k * count, base + (k + 1) * count) for k in range(ups)]
        lows = [jnp.where(high_first, got_two[r, :], got_one[r, :]) for r in rows]
        highs = [jnp.where(high_first, got_one[r, :], got_two[r, :]) for r in rows[:downs]]
        joined(state, lows, highs, is_first, is_last, spans)
        parts += level_one(state) if count == BLOCK else level_two(state, is_last)
    parts.append(blank[...])
    whole = jnp.concatenate(parts, axis=0)
    both[...] = whole
    turned = whole.T
    up_first, _ = here("gy")
    up[...] = turned[LANES - EDGE :, :]
    down[...] = turned[:EDGE, :]
    send_one[...] = jnp.where(up_first, turned[LANES - EDGE :, :], turned[:EDGE, :])
    send_two[...] = jnp.where(up_first, turned[:EDGE, :], turned[LANES - EDGE :, :])


def dot(a, b):
    return jnp.dot(a, b, precision=lax.Precision.HIGHEST, preferred_element_type=jnp.float32)


def y_main_kernel(both, mains, out):
    cells = BLOCK * BLOCK
    out[:cells, :] = dot(both[:cells, :], mains[0])
    out[cells:, :] = dot(both[cells : cells + cells // 4, :], mains[1])


def y_kernel(main, got_one, got_two, up, down, edges, out, block, sems):
    where = lax.axis_index("gy")
    is_first, is_last = where == 0, where == lax.axis_size("gy") - 1
    cells, half = BLOCK * BLOCK, BLOCK // 2
    _, high_first = here("gy")
    low = jnp.where(high_first, got_two[...], got_one[...])
    high = jnp.where(high_first, got_one[...], got_two[...])
    ends = jnp.concatenate([jnp.where(is_first, down[...], low), jnp.where(is_last, up[...], high)], axis=0).T
    weights = [
        jnp.concatenate(
            [jnp.where(is_first, edges[k, 1], edges[k, 0]), jnp.where(is_last, edges[k, 3], edges[k, 2])], axis=0
        )
        for k in range(2)
    ]
    even = (lax.broadcasted_iota(jnp.int32, (half, LANES), 1) & 1) == 0
    whole = block.reshape(BLOCK, BLOCK, LANES)
    copies = []
    for part in range(2):
        rows = slice(part * cells // 2, (part + 1) * cells // 2)
        one = main[rows, :] + dot(ends[rows, :], weights[0])
        rows = slice(cells + part * cells // 8, cells + (part + 1) * cells // 8)
        two = main[rows, :] + dot(ends[rows, :], weights[1])
        for z in range(half):
            block[pl.ds(part * half + z, BLOCK, stride=BLOCK), :] = one[z * BLOCK : (z + 1) * BLOCK, :]
        for z in range(half // 2):
            at = pl.ds(part * half + 2 * z, half, stride=2 * BLOCK)
            block[at, :] = jnp.where(even, two[z * half : (z + 1) * half, :], block[at, :])
        span = pl.ds(part * half, half)
        copies.append(pltpu.make_async_copy(whole.at[:, span, :], out.at[:, span, :], sems.at[part]))
        copies[-1].start()
    for copy in copies:
        copy.wait()


def near(shape):
    return pltpu.VMEM(shape, jnp.float32)


def call(kernel, shapes, *args, flops=None):
    args = [pltpu.with_memory_space_constraint(a, pltpu.VMEM) for a in args]
    cost = None if flops is None else pl.CostEstimate(flops=flops, bytes_accessed=4096, transcendentals=0)
    return pl.pallas_call(kernel, out_shape=shapes, cost_estimate=cost)(*args)


def exchange(up, down, axis):
    count = lax.axis_size(axis)
    forward = [(i, i + 1) for i in range(count - 1)]
    backward = [(target, source) for source, target in forward]
    high = lax.ppermute(down, axis, backward)
    low = lax.ppermute(up, axis, forward)
    return low, high


def exchange_lines(one, two, axis):
    names = ("gx", "gy", "gz")
    sizes = [lax.axis_size(name) for name in names]
    dim = names.index(axis)
    steps = ([], [])
    for source, at in enumerate(itertools.product(*[range(size) for size in sizes])):
        up_first = swapped(axis, *at) and at[dim] % 2 == 1
        for step, upward in enumerate((up_first, not up_first)):
            to = list(at)
            to[dim] += 1 if upward else -1
            if 0 <= to[dim] < sizes[dim]:
                steps[step].append((source, (to[0] * sizes[1] + to[1]) * sizes[2] + to[2]))
    one = lax.ppermute(one, names, steps[0])
    two = lax.ppermute(two, names, steps[1])
    return one, two


def on_device(field):
    cells, half = BLOCK * BLOCK, BLOCK // 2
    (blank,) = call(blank_kernel, [near((64, LANES))], flops=10**8)
    (down,) = call(x_start_kernel, [near((len(DOWN), BLOCK, LANES))], field, blank)
    low, high = exchange(field, down, "gx")
    one, two, send_one, send_two = call(
        x_kernel,
        [
            near((cells, LANES)),
            near((half * BLOCK, LANES)),
            near((3 * BLOCK + 7 * half, LANES)),
            near((3 * BLOCK + 7 * half, LANES)),
        ],
        field,
        low,
        high,
    )
    got_one, got_two = exchange_lines(send_one, send_two, "gz")
    wide = cells + 128
    both, up, down, send_one, send_two = call(
        z_kernel, [near((wide, LANES))] + [near((EDGE, wide))] * 4, one, two, got_one, got_two, blank
    )
    got_one, got_two = exchange_lines(send_one, send_two, "gy")
    (main,) = call(
        y_main_kernel, [near((cells + cells // 4, LANES))], both, jnp.asarray(MAINS), flops=10**7
    )
    out = pl.pallas_call(
        y_kernel,
        out_shape=jax.ShapeDtypeStruct((BLOCK, BLOCK, LANES), jnp.float32),
        out_specs=pl.BlockSpec(memory_space=pl.ANY),
        scratch_shapes=[pltpu.VMEM((cells, LANES), jnp.float32), pltpu.SemaphoreType.DMA((2,))],
        name="y_kernel",
    )(*(pltpu.with_memory_space_constraint(a, pltpu.VMEM) for a in (main, got_one, got_two, up, down, jnp.asarray(EDGES))))
    return out


def solution(mesh):
    placed = (P("gx", "gz", "gy"),)
    return jax.shard_map(
        on_device, mesh=mesh, in_specs=placed, out_specs=P("gx", "gz", "gy"), check_vma=False
    )
```

```python
import itertools

import jax
import jax.numpy as jnp
import numpy as np
from jax import lax
from jax.experimental import pallas as pl
from jax.experimental.pallas import tpu as pltpu
from jax.sharding import PartitionSpec as P

ALPHA = -1.586134342
BETA = -0.05298011854
GAMMA = 0.8829110762
DELTA = 0.4435068522
ZETA = 1.149604398

BLOCK = 16
LANES = 128
EDGE = 16
NEAR = {"gx": (1, 1), "gz": (1, 2), "gy": (2, 2)}


STEPS = (ALPHA, BETA, GAMMA, DELTA)


def advance(state, step, index):
    before = max(step - 2, -1) if step > 1 else -1
    side = step - 1
    state[step, index] = state[before, index] + STEPS[step] * (state[side, index - 1] + state[side, index + 1])


def lift(state, spans):
    for step, (first, last) in enumerate(spans):
        for index in range(first, last + 1, 2):
            if (step, index) not in state:
                advance(state, step, index)


UP = ((-1, 15), (-1, 14), (0, 13), (1, 12), (2, 11), (3, 10), (3, 8))
DOWN = ((-1, 0), (0, 1), (1, 2), (2, 3), (3, 4))
MIRROR_LOW = ((-1, 1), (-1, 2), (0, 3), (1, 4), (2, 5), (3, 6), (3, 8))
MIRROR_HIGH = ((-1, 14), (0, 13), (1, 12), (2, 11), (3, 10))
INNER = ((1, 13), (2, 12), (3, 11), (4, 10))
BOTH = ((-1, 15), (-2, 16), (-3, 17), (-4, 18))
ONE = ((-1, 15), (-2, 16), (-1, 15), (0, 14))


def started(rows):
    state = {(-1, i): rows[i] for i in range(BLOCK)}
    lift(state, INNER)
    return state


def joined(state, low, high, is_first, is_last, spans):
    for k, value in enumerate(low):
        step, index = UP[k]
        state[step, index - BLOCK] = jnp.where(is_first, state[MIRROR_LOW[k]], value)
    for k, value in enumerate(high):
        step, index = DOWN[k]
        state[step, index + BLOCK] = jnp.where(is_last, state[MIRROR_HIGH[k]], value)
    lift(state, spans)
    return state


def level_one(state):
    return [state[2, i] * (1.0 / ZETA) if i & 1 else state[3, i] * ZETA for i in range(BLOCK)]


def level_two(state, is_last):
    half = BLOCK // 2
    coarse = {(-1, i): state[3, 2 * i] * ZETA for i in range(-4, half + 3)}
    for j in range(3):
        coarse[-1, half + j] = jnp.where(is_last, coarse[-1, half - 2 - j], coarse[-1, half + j])
    lift(coarse, ((-3, half + 1), (-2, half), (-1, half - 1), (0, half - 2)))
    return [coarse[2, i] * (1.0 / ZETA) if i & 1 else coarse[3, i] * ZETA for i in range(half)]


def lift_matrix(padded):
    even, odd = padded[0::2], padded[1::2]
    odd = odd[:-1] + ALPHA * (even[:-1] + even[1:])
    even = even[1:-1] + BETA * (odd[:-1] + odd[1:])
    odd = odd[1:-1] + GAMMA * (even[:-1] + even[1:])
    even = even[1:-1] + DELTA * (odd[:-1] + odd[1:])
    out = np.zeros((2 * len(even), padded.shape[1]))
    out[0::2] = even * ZETA
    out[1::2] = odd[1:] / ZETA
    return out


def y_matrices():
    n, wide = LANES, 24
    size = n + 2 * wide
    eye = np.eye(size)
    own = eye[wide : wide + n]

    def levels(ext, last):
        one = lift_matrix(ext)
        low = one[0::2]
        if last:
            half = n // 2
            low = low.copy()
            for j in range(8):
                low[10 + half + j] = low[10 + half - 2 - j]
        two = lift_matrix(low[: len(low) - len(low) % 2])
        fine = np.zeros((n, size))
        fine[0::2] = two[6 : 6 + n // 2]
        return one[20 : 20 + n], fine

    inner = levels(eye, False)
    left = eye.copy()
    left[:wide] = own[1 : wide + 1][::-1]
    first = levels(left, False)
    right = eye.copy()
    right[wide + n :] = own[n - 1 - wide : n - 1][::-1]
    final = levels(right, True)
    mains, edges = [], []
    for a, b, c in zip(inner, first, final):
        a, b, c = a.T, b.T, c.T
        mid = a[wide : wide + n]
        edges.append(
            np.stack(
                [
                    a[wide - EDGE : wide],
                    (b - a)[wide : wide + EDGE],
                    a[wide + n : wide + n + EDGE],
                    (c - a)[wide + n - EDGE : wide + n],
                ]
            )
        )
        mains.append(mid)
    return np.stack(mains).astype(np.float32), np.stack(edges).astype(np.float32)


MAINS, EDGES = y_matrices()


def swapped(axis, gx, gy, gz):
    if axis == "gx":
        return (gy < NEAR["gx"][0]) & (gz < NEAR["gx"][1])
    if axis == "gz":
        return (gy < NEAR["gz"][0]) & (gx < NEAR["gz"][1])
    return (gz < NEAR["gy"][0]) & (gx < NEAR["gy"][1])


def here(axis):
    at = {name: lax.axis_index(name) for name in ("gx", "gy", "gz")}
    swap = swapped(axis, **at)
    odd = lax.rem(at[axis], 2) == 1
    return swap & odd, jnp.logical_or(jnp.logical_not(swap), odd)


def blank_kernel(blank):
    blank[...] = jnp.zeros(blank.shape, jnp.float32)


def x_start_kernel(field, blank, send_two):
    state = started({i: field[i] for i in range(BLOCK)})
    up_first, _ = here("gx")
    swap = swapped("gx", *(lax.axis_index(name) for name in ("gx", "gy", "gz")))
    goes_up = swap & jnp.logical_not(up_first)
    for k, key in enumerate(UP):
        send_two[k] = jnp.where(goes_up, state[key], state[DOWN[min(k, len(DOWN) - 1)]])


def x_kernel(field, got_one, got_two, one, two, send_one, send_two):
    where = lax.axis_index("gx")
    is_first, is_last = where == 0, where == lax.axis_size("gx") - 1
    half = BLOCK // 2
    up_first, _ = here("gx")
    beside = started({i: got_one[i] for i in range(BLOCK)})
    state = started({i: field[i] for i in range(BLOCK)})
    lows = [jnp.where(up_first, got_two[k], beside[key]) for k, key in enumerate(UP)]
    highs = [jnp.where(up_first, beside[key], got_two[k]) for k, key in enumerate(DOWN)]
    joined(state, lows, highs, is_first, is_last, BOTH)
    for i, row in enumerate(level_one(state)):
        one[i * BLOCK : (i + 1) * BLOCK, :] = row
    for i, row in enumerate(level_two(state, is_last)):
        two[i * BLOCK : (i + 1) * BLOCK, :] = row
    up_first, _ = here("gz")
    for source, count, base, ups, downs in ((one, BLOCK, 0, 3, 2), (two, half, 3 * BLOCK, 7, 5)):
        state = started({i: source[pl.ds(i, count, stride=BLOCK), :] for i in range(BLOCK)})
        for k in range(ups):
            rows = slice(base + k * count, base + (k + 1) * count)
            up, down = state[UP[k]], state[DOWN[min(k, downs - 1)]]
            send_one[rows, :] = jnp.where(up_first, up, down)
            send_two[rows, :] = jnp.where(up_first, down, up)


def z_kernel(one, two, got_one, got_two, blank, both, up, down, send_one, send_two):
    where = lax.axis_index("gz")
    is_first, is_last = where == 0, where == lax.axis_size("gz") - 1
    half = BLOCK // 2
    _, high_first = here("gz")
    parts = []
    for source, count, base, ups, downs, spans in ((one, BLOCK, 0, 3, 2, ONE), (two, half, 3 * BLOCK, 7, 5, BOTH)):
        state = started({i: source[pl.ds(i, count, stride=BLOCK), :] for i in range(BLOCK)})
        rows = [slice(base + k * count, base + (k + 1) * count) for k in range(ups)]
        lows = [jnp.where(high_first, got_two[r, :], got_one[r, :]) for r in rows]
        highs = [jnp.where(high_first, got_one[r, :], got_two[r, :]) for r in rows[:downs]]
        joined(state, lows, highs, is_first, is_last, spans)
        parts += level_one(state) if count == BLOCK else level_two(state, is_last)
    parts.append(blank[...])
    whole = jnp.concatenate(parts, axis=0)
    both[...] = whole
    turned = whole.T
    up_first, _ = here("gy")
    up[...] = turned[LANES - EDGE :, :]
    down[...] = turned[:EDGE, :]
    send_one[...] = jnp.where(up_first, turned[LANES - EDGE :, :], turned[:EDGE, :])
    send_two[...] = jnp.where(up_first, turned[:EDGE, :], turned[LANES - EDGE :, :])


def dot(a, b):
    return jnp.dot(a, b, precision=lax.Precision.HIGHEST, preferred_element_type=jnp.float32)


def y_main_kernel(both, mains, out):
    cells = BLOCK * BLOCK
    out[:cells, :] = dot(both[:cells, :], mains[0])
    out[cells:, :] = dot(both[cells : cells + cells // 4, :], mains[1])


def y_kernel(main, got_one, got_two, up, down, edges, out, block, sems):
    where = lax.axis_index("gy")
    is_first, is_last = where == 0, where == lax.axis_size("gy") - 1
    cells, half = BLOCK * BLOCK, BLOCK // 2
    _, high_first = here("gy")
    low = jnp.where(high_first, got_two[...], got_one[...])
    high = jnp.where(high_first, got_one[...], got_two[...])
    ends = jnp.concatenate([jnp.where(is_first, down[...], low), jnp.where(is_last, up[...], high)], axis=0).T
    weights = [
        jnp.concatenate(
            [jnp.where(is_first, edges[k, 1], edges[k, 0]), jnp.where(is_last, edges[k, 3], edges[k, 2])], axis=0
        )
        for k in range(2)
    ]
    even = (lax.broadcasted_iota(jnp.int32, (half, LANES), 1) & 1) == 0
    whole = block.reshape(BLOCK, BLOCK, LANES)
    copies = []
    for part in range(2):
        rows = slice(part * cells // 2, (part + 1) * cells // 2)
        one = main[rows, :] + dot(ends[rows, :], weights[0])
        rows = slice(cells + part * cells // 8, cells + (part + 1) * cells // 8)
        two = main[rows, :] + dot(ends[rows, :], weights[1])
        for z in range(half):
            block[pl.ds(part * half + z, BLOCK, stride=BLOCK), :] = one[z * BLOCK : (z + 1) * BLOCK, :]
        for z in range(half // 2):
            at = pl.ds(part * half + 2 * z, half, stride=2 * BLOCK)
            block[at, :] = jnp.where(even, two[z * half : (z + 1) * half, :], block[at, :])
        span = pl.ds(part * half, half)
        copies.append(pltpu.make_async_copy(whole.at[:, span, :], out.at[:, span, :], sems.at[part]))
        copies[-1].start()
    for copy in copies:
        copy.wait()


def near(shape):
    return pltpu.VMEM(shape, jnp.float32)


def call(kernel, shapes, *args, flops=None):
    args = [pltpu.with_memory_space_constraint(a, pltpu.VMEM) for a in args]
    cost = None if flops is None else pl.CostEstimate(flops=flops, bytes_accessed=4096, transcendentals=0)
    return pl.pallas_call(kernel, out_shape=shapes, cost_estimate=cost)(*args)


def exchange_lines(one, two, axis):
    names = ("gx", "gy", "gz")
    sizes = [lax.axis_size(name) for name in names]
    dim = names.index(axis)
    steps = ([], [])
    for source, at in enumerate(itertools.product(*[range(size) for size in sizes])):
        if swapped(axis, *at):
            up_first = at[dim] % 2 == 1
        else:
            up_first = axis == "gx"
        for step, upward in enumerate((up_first, not up_first)):
            to = list(at)
            to[dim] += 1 if upward else -1
            if 0 <= to[dim] < sizes[dim]:
                steps[step].append((source, (to[0] * sizes[1] + to[1]) * sizes[2] + to[2]))
    one = lax.ppermute(one, names, steps[0])
    two = lax.ppermute(two, names, steps[1])
    return one, two


def on_device(field):
    cells, half = BLOCK * BLOCK, BLOCK // 2
    (blank,) = call(blank_kernel, [near((64, LANES))], flops=10**8)
    (send_two,) = call(x_start_kernel, [near((len(UP), BLOCK, LANES))], field, blank)
    got_one, got_two = exchange_lines(field, send_two, "gx")
    one, two, send_one, send_two = call(
        x_kernel,
        [
            near((cells, LANES)),
            near((half * BLOCK, LANES)),
            near((3 * BLOCK + 7 * half, LANES)),
            near((3 * BLOCK + 7 * half, LANES)),
        ],
        field,
        got_one,
        got_two,
    )
    got_one, got_two = exchange_lines(send_one, send_two, "gz")
    wide = cells + 128
    both, up, down, send_one, send_two = call(
        z_kernel, [near((wide, LANES))] + [near((EDGE, wide))] * 4, one, two, got_one, got_two, blank
    )
    got_one, got_two = exchange_lines(send_one, send_two, "gy")
    (main,) = call(
        y_main_kernel, [near((cells + cells // 4, LANES))], both, jnp.asarray(MAINS), flops=10**7
    )
    out = pl.pallas_call(
        y_kernel,
        out_shape=jax.ShapeDtypeStruct((BLOCK, BLOCK, LANES), jnp.float32),
        out_specs=pl.BlockSpec(memory_space=pl.ANY),
        scratch_shapes=[pltpu.VMEM((cells, LANES), jnp.float32), pltpu.SemaphoreType.DMA((2,))],
        name="y_kernel",
    )(*(pltpu.with_memory_space_constraint(a, pltpu.VMEM) for a in (main, got_one, got_two, up, down, jnp.asarray(EDGES))))
    return out


def solution(mesh):
    placed = (P("gx", "gz", "gy"),)
    return jax.shard_map(
        on_device, mesh=mesh, in_specs=placed, out_specs=P("gx", "gz", "gy"), check_vma=False
    )
```

```python
import itertools

import jax
import jax.numpy as jnp
import numpy as np
from jax import lax
from jax.experimental import pallas as pl
from jax.experimental.pallas import tpu as pltpu
from jax.sharding import PartitionSpec as P

ALPHA = -1.586134342
BETA = -0.05298011854
GAMMA = 0.8829110762
DELTA = 0.4435068522
ZETA = 1.149604398

BLOCK = 16
LANES = 128
EDGE = 16
NEAR = {"gx": (8, 8), "gz": (1, 2), "gy": 2}


STEPS = (ALPHA, BETA, GAMMA, DELTA)


def advance(state, step, index):
    before = max(step - 2, -1) if step > 1 else -1
    side = step - 1
    state[step, index] = state[before, index] + STEPS[step] * (state[side, index - 1] + state[side, index + 1])


def lift(state, spans):
    for step, (first, last) in enumerate(spans):
        for index in range(first, last + 1, 2):
            if (step, index) not in state:
                advance(state, step, index)


UP = ((-1, 15), (-1, 14), (0, 13), (1, 12), (2, 11), (3, 10), (3, 8))
DOWN = ((-1, 0), (0, 1), (1, 2), (2, 3), (3, 4))
MIRROR_LOW = ((-1, 1), (-1, 2), (0, 3), (1, 4), (2, 5), (3, 6), (3, 8))
MIRROR_HIGH = ((-1, 14), (0, 13), (1, 12), (2, 11), (3, 10))
INNER = ((1, 13), (2, 12), (3, 11), (4, 10))
BOTH = ((-1, 15), (-2, 16), (-3, 17), (-4, 18))
ONE = ((-1, 15), (-2, 16), (-1, 15), (0, 14))


def started(rows):
    state = {(-1, i): rows[i] for i in range(BLOCK)}
    lift(state, INNER)
    return state


def joined(state, low, high, is_first, is_last, spans):
    for k, value in enumerate(low):
        step, index = UP[k]
        state[step, index - BLOCK] = jnp.where(is_first, state[MIRROR_LOW[k]], value)
    for k, value in enumerate(high):
        step, index = DOWN[k]
        state[step, index + BLOCK] = jnp.where(is_last, state[MIRROR_HIGH[k]], value)
    lift(state, spans)
    return state


def level_one(state):
    return [state[2, i] * (1.0 / ZETA) if i & 1 else state[3, i] * ZETA for i in range(BLOCK)]


def level_two(state, is_last):
    half = BLOCK // 2
    coarse = {(-1, i): state[3, 2 * i] * ZETA for i in range(-4, half + 3)}
    for j in range(3):
        coarse[-1, half + j] = jnp.where(is_last, coarse[-1, half - 2 - j], coarse[-1, half + j])
    lift(coarse, ((-3, half + 1), (-2, half), (-1, half - 1), (0, half - 2)))
    return [coarse[2, i] * (1.0 / ZETA) if i & 1 else coarse[3, i] * ZETA for i in range(half)]


def lift_matrix(padded):
    even, odd = padded[0::2], padded[1::2]
    odd = odd[:-1] + ALPHA * (even[:-1] + even[1:])
    even = even[1:-1] + BETA * (odd[:-1] + odd[1:])
    odd = odd[1:-1] + GAMMA * (even[:-1] + even[1:])
    even = even[1:-1] + DELTA * (odd[:-1] + odd[1:])
    out = np.zeros((2 * len(even), padded.shape[1]))
    out[0::2] = even * ZETA
    out[1::2] = odd[1:] / ZETA
    return out


def y_matrices():
    n, wide = LANES, 24
    size = n + 2 * wide
    eye = np.eye(size)
    own = eye[wide : wide + n]

    def levels(ext, last):
        one = lift_matrix(ext)
        low = one[0::2]
        if last:
            half = n // 2
            low = low.copy()
            for j in range(8):
                low[10 + half + j] = low[10 + half - 2 - j]
        two = lift_matrix(low[: len(low) - len(low) % 2])
        fine = np.zeros((n, size))
        fine[0::2] = two[6 : 6 + n // 2]
        return one[20 : 20 + n], fine

    inner = levels(eye, False)
    left = eye.copy()
    left[:wide] = own[1 : wide + 1][::-1]
    first = levels(left, False)
    right = eye.copy()
    right[wide + n :] = own[n - 1 - wide : n - 1][::-1]
    final = levels(right, True)
    mains, edges = [], []
    for a, b, c in zip(inner, first, final):
        a, b, c = a.T, b.T, c.T
        mid = a[wide : wide + n]
        edges.append(
            np.stack(
                [
                    a[wide - EDGE : wide],
                    (b - a)[wide : wide + EDGE],
                    a[wide + n : wide + n + EDGE],
                    (c - a)[wide + n - EDGE : wide + n],
                ]
            )
        )
        mains.append(mid)
    return np.stack(mains).astype(np.float32), np.stack(edges).astype(np.float32)


MAINS, EDGES = y_matrices()


def swapped(axis, gx, gy, gz):
    if axis == "gx":
        return (gy < NEAR["gx"][0]) & (gz < NEAR["gx"][1])
    if axis == "gz":
        return (gy < NEAR["gz"][0]) & (gx < NEAR["gz"][1])
    return gz + gx < NEAR["gy"]


def here(axis):
    at = {name: lax.axis_index(name) for name in ("gx", "gy", "gz")}
    swap = swapped(axis, **at)
    odd = lax.rem(at[axis], 2) == 1
    return swap & odd, jnp.logical_or(jnp.logical_not(swap), odd)


def blank_kernel(blank):
    blank[...] = jnp.zeros(blank.shape, jnp.float32)


def x_start_kernel(field, blank, send_two):
    state = started({i: field[i] for i in range(BLOCK)})
    up_first, _ = here("gx")
    swap = swapped("gx", *(lax.axis_index(name) for name in ("gx", "gy", "gz")))
    goes_up = swap & jnp.logical_not(up_first)
    for k, key in enumerate(UP):
        send_two[k] = jnp.where(goes_up, state[key], state[DOWN[min(k, len(DOWN) - 1)]])


def x_kernel(field, got_one, got_two, one, two, send_one, send_two):
    where = lax.axis_index("gx")
    is_first, is_last = where == 0, where == lax.axis_size("gx") - 1
    half = BLOCK // 2
    up_first, _ = here("gx")
    beside = started({i: got_one[i] for i in range(BLOCK)})
    state = started({i: field[i] for i in range(BLOCK)})
    lows = [jnp.where(up_first, got_two[k], beside[key]) for k, key in enumerate(UP)]
    highs = [jnp.where(up_first, beside[key], got_two[k]) for k, key in enumerate(DOWN)]
    joined(state, lows, highs, is_first, is_last, BOTH)
    for i, row in enumerate(level_one(state)):
        one[i * BLOCK : (i + 1) * BLOCK, :] = row
    for i, row in enumerate(level_two(state, is_last)):
        two[i * BLOCK : (i + 1) * BLOCK, :] = row
    up_first, _ = here("gz")
    for source, count, base, ups, downs in ((one, BLOCK, 0, 3, 2), (two, half, 3 * BLOCK, 7, 5)):
        state = started({i: source[pl.ds(i, count, stride=BLOCK), :] for i in range(BLOCK)})
        for k in range(ups):
            rows = slice(base + k * count, base + (k + 1) * count)
            up, down = state[UP[k]], state[DOWN[min(k, downs - 1)]]
            send_one[rows, :] = jnp.where(up_first, up, down)
            send_two[rows, :] = jnp.where(up_first, down, up)


def z_kernel(one, two, got_one, got_two, blank, both, up, down, send_one, send_two):
    where = lax.axis_index("gz")
    is_first, is_last = where == 0, where == lax.axis_size("gz") - 1
    half = BLOCK // 2
    _, high_first = here("gz")
    parts = []
    for source, count, base, ups, downs, spans in ((one, BLOCK, 0, 3, 2, ONE), (two, half, 3 * BLOCK, 7, 5, BOTH)):
        state = started({i: source[pl.ds(i, count, stride=BLOCK), :] for i in range(BLOCK)})
        rows = [slice(base + k * count, base + (k + 1) * count) for k in range(ups)]
        lows = [jnp.where(high_first, got_two[r, :], got_one[r, :]) for r in rows]
        highs = [jnp.where(high_first, got_one[r, :], got_two[r, :]) for r in rows[:downs]]
        joined(state, lows, highs, is_first, is_last, spans)
        parts += level_one(state) if count == BLOCK else level_two(state, is_last)
    parts.append(blank[...])
    whole = jnp.concatenate(parts, axis=0)
    both[...] = whole
    turned = whole.T
    up_first, _ = here("gy")
    up[...] = turned[LANES - EDGE :, :]
    down[...] = turned[:EDGE, :]
    send_one[...] = jnp.where(up_first, turned[LANES - EDGE :, :], turned[:EDGE, :])
    send_two[...] = jnp.where(up_first, turned[:EDGE, :], turned[LANES - EDGE :, :])


def dot(a, b):
    return jnp.dot(a, b, precision=lax.Precision.HIGHEST, preferred_element_type=jnp.float32)


def split(v):
    high = v.astype(jnp.bfloat16)
    rest = v - high.astype(jnp.float32)
    middle = rest.astype(jnp.bfloat16)
    return high, middle, (rest - middle.astype(jnp.float32)).astype(jnp.bfloat16)


def turned_dot(a, b):
    return lax.dot_general(a, b, (((0,), (0,)), ((), ())), preferred_element_type=jnp.float32)


def y_main_kernel(both, mains, out):
    cells = BLOCK * BLOCK
    out[:cells, :] = dot(both[:cells, :], mains[0])
    out[cells:, :] = dot(both[cells : cells + cells // 4, :], mains[1])


def y_kernel(main, got_one, got_two, up, down, edges, out, block, sems):
    where = lax.axis_index("gy")
    is_first, is_last = where == 0, where == lax.axis_size("gy") - 1
    cells, half = BLOCK * BLOCK, BLOCK // 2
    _, high_first = here("gy")
    low = jnp.where(high_first, got_two[...], got_one[...])
    high = jnp.where(high_first, got_one[...], got_two[...])
    ends = jnp.concatenate([jnp.where(is_first, down[...], low), jnp.where(is_last, up[...], high)], axis=0)
    big, mid, small = split(ends)
    ends = jnp.concatenate([big, big, mid, mid, big, small], axis=0)
    weights = []
    for k in range(2):
        big, mid, small = split(
            jnp.concatenate(
                [jnp.where(is_first, edges[k, 1], edges[k, 0]), jnp.where(is_last, edges[k, 3], edges[k, 2])], axis=0
            )
        )
        weights.append(jnp.concatenate([big, mid, big, mid, small, big], axis=0))
    coarse = main[cells:, :] + turned_dot(ends[:, cells:], weights[1])[: cells // 4, :]
    even = (lax.broadcasted_iota(jnp.int32, (half, LANES), 1) & 1) == 0
    whole = block.reshape(BLOCK, BLOCK, LANES)
    copies = []
    for part in range(2):
        rows = slice(part * cells // 2, (part + 1) * cells // 2)
        one = main[rows, :] + turned_dot(ends[:, rows], weights[0])
        two = coarse[part * cells // 8 : (part + 1) * cells // 8, :]
        for z in range(half):
            block[pl.ds(part * half + z, BLOCK, stride=BLOCK), :] = one[z * BLOCK : (z + 1) * BLOCK, :]
        for z in range(half // 2):
            at = pl.ds(part * half + 2 * z, half, stride=2 * BLOCK)
            block[at, :] = jnp.where(even, two[z * half : (z + 1) * half, :], block[at, :])
        span = pl.ds(part * half, half)
        copies.append(pltpu.make_async_copy(whole.at[:, span, :], out.at[:, span, :], sems.at[part]))
        copies[-1].start()
    for copy in copies:
        copy.wait()


def near(shape):
    return pltpu.VMEM(shape, jnp.float32)


def call(kernel, shapes, *args, flops=None):
    args = [pltpu.with_memory_space_constraint(a, pltpu.VMEM) for a in args]
    cost = None if flops is None else pl.CostEstimate(flops=flops, bytes_accessed=4096, transcendentals=0)
    return pl.pallas_call(kernel, out_shape=shapes, cost_estimate=cost)(*args)


def exchange_lines(one, two, axis):
    names = ("gx", "gy", "gz")
    sizes = [lax.axis_size(name) for name in names]
    dim = names.index(axis)
    steps = ([], [])
    for source, at in enumerate(itertools.product(*[range(size) for size in sizes])):
        if swapped(axis, *at):
            up_first = at[dim] % 2 == 1
        else:
            up_first = axis == "gx"
        for step, upward in enumerate((up_first, not up_first)):
            to = list(at)
            to[dim] += 1 if upward else -1
            if 0 <= to[dim] < sizes[dim]:
                steps[step].append((source, (to[0] * sizes[1] + to[1]) * sizes[2] + to[2]))
    one = lax.ppermute(one, names, steps[0])
    two = lax.ppermute(two, names, steps[1])
    return one, two


def on_device(field):
    cells, half = BLOCK * BLOCK, BLOCK // 2
    (blank,) = call(blank_kernel, [near((64, LANES))], flops=10**8)
    (send_two,) = call(x_start_kernel, [near((len(UP), BLOCK, LANES))], field, blank)
    got_one, got_two = exchange_lines(field, send_two, "gx")
    one, two, send_one, send_two = call(
        x_kernel,
        [
            near((cells, LANES)),
            near((half * BLOCK, LANES)),
            near((3 * BLOCK + 7 * half, LANES)),
            near((3 * BLOCK + 7 * half, LANES)),
        ],
        field,
        got_one,
        got_two,
    )
    got_one, got_two = exchange_lines(send_one, send_two, "gz")
    wide = cells + 128
    both, up, down, send_one, send_two = call(
        z_kernel, [near((wide, LANES))] + [near((EDGE, wide))] * 4, one, two, got_one, got_two, blank
    )
    got_one, got_two = exchange_lines(send_one, send_two, "gy")
    (main,) = call(
        y_main_kernel, [near((cells + cells // 4, LANES))], both, jnp.asarray(MAINS), flops=10**7
    )
    out = pl.pallas_call(
        y_kernel,
        out_shape=jax.ShapeDtypeStruct((BLOCK, BLOCK, LANES), jnp.float32),
        out_specs=pl.BlockSpec(memory_space=pl.ANY),
        scratch_shapes=[pltpu.VMEM((cells, LANES), jnp.float32), pltpu.SemaphoreType.DMA((2,))],
        name="y_kernel",
    )(*(pltpu.with_memory_space_constraint(a, pltpu.VMEM) for a in (main, got_one, got_two, up, down, jnp.asarray(EDGES))))
    return out


def solution(mesh):
    placed = (P("gx", "gz", "gy"),)
    return jax.shard_map(
        on_device, mesh=mesh, in_specs=placed, out_specs=P("gx", "gz", "gy"), check_vma=False
    )
```
